32 devices in a mesh: rp: 2 (over x), pb: 16 (over z, y, core).
Axes of the slice: x: 2, y: 2, z: 4, core: 2. Of those that a mesh axis runs over, the one named last changes fastest.
Arguments:
- wannier_g: bfloat16 [2, 1024, 32, 1152], P(None, 'rp', 'pb'), may hold values from -0.19921875 to 0.19921875
- rp_coords: int32 [3, 1024], replicated, may hold values from -8 to 8
- q_coords: int32 [3, 64], P(None, ('rp', 'pb')), may hold values from 0 to 15
- k_index: int32 [1], replicated, may hold values from 0 to 7
- k_vectors: bfloat16 [8, 2, 32, 32], replicated, may hold values from -0.75 to 0.75
- kq_vectors: bfloat16 [64, 2, 32, 32], P(('rp', 'pb')), may hold values from -0.75 to 0.75
- modes: bfloat16 [64, 2, 36, 36], P(('rp', 'pb')), may hold values from -0.75 to 0.75
Outputs:
- rotated: float32 [64, 2, 32, 1152], P(('rp', 'pb'))
The draws below stay inside these ranges and needn't reach their ends.
All inputs are finite; a program needn't handle non-finite values.
Results may differ from the reference program's by a relative error of at most 0.0054.
Values may be sent and summed in bfloat16 or wider, within the bound.
A program may use at most 64 MiB of HBM per device.

```python
import math
import jax
import jax.numpy as jnp
from jax import lax

NB = 32
NM = 36
NR = 1024
NK = 16
KB = 8
Q_DEV = 2
Q = 64
N_RP = 2
N_PB = 16


def with_ends(entries, stream_key, least, largest):
    longest = entries.shape.index(max(entries.shape))
    spots = []
    for shift in (0, 1):
        where = [jax.random.randint(jax.random.fold_in(stream_key, axis), (), 0, length) for axis, length in enumerate(entries.shape)]
        where[longest] = (where[longest] + shift) % entries.shape[longest]
        spots.append(tuple(where))
    return entries.at[spots[0]].set(least).at[spots[1]].set(largest)


def levels(own_key, dims, cuts, low, largest):
    def one(axis_at, parts):
        heights = jax.random.uniform(jax.random.fold_in(jax.random.fold_in(own_key, 6), axis_at), (parts,), jnp.float32, low / len(cuts), largest / len(cuts))
        return jnp.repeat(jnp.exp(heights), dims[axis_at] // parts).reshape((-1,) + (1,) * (len(dims) - axis_at - 1))

    factor_of = one(*cuts[0])
    for cut in cuts[1:]:
        factor_of = factor_of * one(*cut)
    return factor_of


def centred(key, extent, width, most, split=(), dtype=jnp.bfloat16):
    values = width * jax.random.normal(key, extent, jnp.float32)
    if split:
        values = values * levels(key, extent, split, -0.22, 0.18)
    return jnp.clip(values, -most, most).astype(dtype)


def setup_inputs(seed: int = 0) -> dict:
    streams_of = jax.random.split(jax.random.key(seed), 8)
    return {
        "wannier_g": centred(streams_of[0], (2, NR, NB, NB * NM), 0.03, 0.19921875, ((1, 2), (2, 16))),
        "rp_coords": with_ends(jax.random.randint(streams_of[1], (3, NR), -8, 9), jax.random.fold_in(streams_of[1], 1), -8, 8).astype(jnp.int32),
        "q_coords": with_ends(jax.random.randint(streams_of[2], (3, Q), 0, NK), jax.random.fold_in(streams_of[2], 1), 0, NK - 1).astype(jnp.int32),
        "k_index": jax.random.randint(streams_of[3], (1,), 0, KB).astype(jnp.int32),
        "k_vectors": centred(streams_of[4], (KB, 2, NB, NB), (2 * NB) ** -0.5, 0.75),
        "kq_vectors": centred(streams_of[5], (Q, 2, NB, NB), (2 * NB) ** -0.5, 0.75, ((0, 32),)),
        "modes": centred(streams_of[6], (Q, 2, NM, NM), (2 * NM) ** -0.5, 0.75, ((0, 32),)),
    }


def phases(q_rows, r_coords):
    turns = jnp.mod(jnp.sum(q_rows[:, :, None] * r_coords[:, None, :], axis=0), NK)
    angle = turns.astype(jnp.float32) * (2.0 * math.pi / NK)
    cosine = jnp.cos(angle).astype(jnp.bfloat16)
    sine = jnp.sin(angle).astype(jnp.bfloat16)
    return jnp.concatenate([cosine, -sine], axis=1), jnp.concatenate([sine, cosine], axis=1)


def rotate(fourier, mode_vecs, unit, kq_vecs):
    count = fourier.shape[0]
    field = fourier.reshape(count, 2, NB, NB, NM).astype(jnp.float32)
    e_real, e_imag = mode_vecs[:, 0], mode_vecs[:, 1]
    e_block = jnp.stack([jnp.stack([e_real, e_imag], 2), jnp.stack([-e_imag, e_real], 2)], 1).astype(jnp.float32)
    by_mode = jnp.einsum("qcmnv,qcvdu->qdmnu", field, e_block).astype(jnp.bfloat16)
    u_real, u_imag = unit[0], unit[1]
    u_block = jnp.stack([jnp.stack([u_real, u_imag], 1), jnp.stack([-u_imag, u_real], 1)], 0).astype(jnp.float32)
    by_band = jnp.einsum("qcmnu,cndj->qdmju", by_mode.astype(jnp.float32), u_block).astype(jnp.bfloat16)
    v_real, v_imag = kq_vecs[:, 0], kq_vecs[:, 1]
    v_block = jnp.stack([jnp.stack([v_real, -v_imag], 2), jnp.stack([v_imag, v_real], 2)], 1).astype(jnp.float32)
    result = jnp.einsum("qcmju,qcmdi->qdiju", by_band.astype(jnp.float32), v_block)
    return result.reshape(count, 2, NB, NB * NM)


def reference(wannier_g, rp_coords, q_coords, k_index, k_vectors, kq_vectors, modes):
    blocks = N_RP * N_PB
    right = wannier_g.reshape(2 * NR, NB * NB * NM)
    unit = lax.dynamic_index_in_dim(k_vectors, k_index[0], 0, keepdims=False)
    q_blocks = q_coords.reshape(3, blocks, Q_DEV).transpose(1, 0, 2)
    mode_blocks = modes.reshape(blocks, Q_DEV, 2, NM, NM)
    kq_blocks = kq_vectors.reshape(blocks, Q_DEV, 2, NB, NB)

    def one_block(items):
        q_rows, mode_vecs, kq_vecs = items
        left_real, left_imag = phases(q_rows, rp_coords)
        f_real = jnp.dot(left_real, right, preferred_element_type=jnp.float32).astype(jnp.bfloat16)
        f_imag = jnp.dot(left_imag, right, preferred_element_type=jnp.float32).astype(jnp.bfloat16)
        fourier = jnp.stack([f_real, f_imag], 1)
        return rotate(fourier, mode_vecs, unit, kq_vecs)

    result = lax.map(one_block, (q_blocks, mode_blocks, kq_blocks))
    return result.reshape(Q, 2, NB, NB * NM)
```

```python
import functools

import jax
import jax.numpy as jnp
import numpy as np
from jax import lax
from jax.experimental import pallas as pl
from jax.experimental.pallas import tpu as pltpu
from jax.sharding import PartitionSpec as P

NK = 16
LANES = 128
MESH = pl.DeviceIdType.MESH
F32 = jnp.float32
BF16 = jnp.bfloat16
ODD = np.linalg.solve(
    np.array([[h, h**3, h**5, h**7] for h in (1.0, 2.0, 3.0, 4.0)]),
    np.sin(np.pi * np.arange(1, 5) / 8.0),
)


def dot(a, b, dims=((1,), (0,))):
    return lax.dot_general(a, b, (dims, ((), ())), preferred_element_type=F32)


def iota(shape, axis):
    return lax.broadcasted_iota(jnp.int32, shape, axis)


def picks(rows, cols, hit):
    return jnp.where(hit(iota((rows, cols), 0), iota((rows, cols), 1)), 1.0, 0.0).astype(BF16)


def wave(turns):
    h = (jnp.abs((turns & (NK - 1)) - NK // 2) - NK // 4).astype(F32)
    s = h * h
    return h * (ODD[0] + s * (ODD[1] + s * (ODD[2] + s * ODD[3])))


def kernel(
    cfg, g_hbm, rp_ref, q_ref, k_ref, kv_ref, v_ref, e_ref, o_ref,
    g_buf, qrow, q_all, send, recv, w_buf, rmat, g_sem, qs_sem, qr_sem, s_sem, r_sem,
):
    n_rp, n_pb, qd, local, M, cols, bands, nu, RB, paired = cfg
    n = n_rp * n_pb
    ip, ib = lax.axis_index("rp"), lax.axis_index("pb")
    me = ip * n_pb + ib
    depth = local * M

    def place(k):
        peer = lax.rem(me + k, n)
        return peer, (lax.div(peer, n_pb), lax.rem(peer, n_pb))

    barrier = pltpu.get_barrier_semaphore()

    def greet(k, c):
        pl.semaphore_signal(barrier, inc=1, device_id=place(k)[1], device_id_type=MESH)
        return c

    lax.fori_loop(1, n, greet, 0)

    tiles = cols // LANES
    loads = []
    for t in range(tiles):
        lanes = pl.ds(LANES * t, LANES)
        src = g_hbm.at[:, :, :, lanes] if paired else g_hbm.at[:, lanes]
        loads.append(pltpu.make_async_copy(src, g_buf.at[t], g_sem.at[t]))
    for c in loads:
        c.start()

    lane = iota((1, LANES), 1)
    row = jnp.zeros((1, LANES), jnp.int32)
    for d in range(3):
        for j in range(qd):
            row = jnp.where(lane == d * qd + j, q_ref[d, j], row)
    qrow[...] = (row & (NK - 1)).astype(F32)

    pl.semaphore_wait(barrier, n - 1)

    def q_copy(k):
        peer, to = place(k)
        return pltpu.make_async_remote_copy(
            src_ref=qrow, dst_ref=q_all.at[me], send_sem=qs_sem.at[peer],
            recv_sem=qr_sem.at[me], device_id=to, device_id_type=MESH,
        )

    def q_start(k, c):
        q_copy(k).start()
        return c

    lax.fori_loop(1, n, q_start, 0)
    q_all[me] = qrow[...]

    own = rp_ref[:, pl.ds(pl.multiple_of(ip * local, LANES), local)] & (NK - 1)
    spread = picks(local, depth, lambda a, b: a == b // M)
    own = dot(own.astype(F32).astype(BF16), spread)
    which = iota((LANES, depth), 0) // qd
    big = jnp.zeros((LANES, depth), F32)
    for d in range(3):
        big = jnp.where(which == d, own[d : d + 1, :], big)
    rmat[...] = big.astype(BF16)

    def q_wait(k, c):
        peer, to = place(k)
        arrived = pltpu.make_async_remote_copy(
            src_ref=qrow, dst_ref=q_all.at[peer], send_sem=qs_sem.at[peer],
            recv_sem=qr_sem.at[peer], device_id=to, device_id_type=MESH,
        )
        arrived.wait_recv()
        q_copy(k).wait_send()
        return c

    lax.fori_loop(1, n, q_wait, 0)

    rows = n * RB
    coords = jnp.broadcast_to(q_all[...], (n, RB, LANES)).reshape(rows, LANES)
    slot = iota((rows, LANES), 0) % RB
    coords = jnp.where(iota((rows, LANES), 1) % qd == slot // (2 * M), coords, 0.0)
    turns = dot(coords.astype(BF16), rmat[...]).astype(jnp.int32)
    slot = iota((rows, 1), 0) % RB
    part = (slot // M) % 2
    keep = (slot % M) == (iota((1, depth), 1) % M)
    left = []
    for shift in (jnp.where(part == 1, 3 * NK // 4, 0), jnp.where(part == 1, 0, NK // 4)):
        left.append(jnp.where(keep, wave(turns + shift), 0.0).astype(BF16))
    left = jnp.concatenate(left, axis=1)

    for t in range(0, tiles, 2):
        parts = []
        for u in range(t, min(t + 2, tiles)):
            loads[u].wait()
            parts.append(g_buf.at[u].reshape(2 * depth, LANES)[...] if paired else g_buf[u])
        right = parts[0] if len(parts) == 1 else jnp.concatenate(parts, axis=1)
        f = dot(left, right).astype(BF16)
        send[:, :, LANES * t : LANES * (t + len(parts))] = f.reshape(n, RB, LANES * len(parts))

    def f_copy(k):
        peer, to = place(k)
        return pltpu.make_async_remote_copy(
            src_ref=send.at[peer], dst_ref=recv.at[me], send_sem=s_sem.at[peer],
            recv_sem=r_sem.at[me], device_id=to, device_id_type=MESH,
        )

    def f_start(k, c):
        f_copy(k).start()
        return c

    lax.fori_loop(1, n, f_start, 0)
    recv[me] = send[me]

    unit = kv_ref[k_ref[0]]
    of_band_t = picks(bands, cols, lambda b, a: (a >= nu * b) & (a < nu * b + nu))
    of_mode_t = picks(nu, cols, lambda b, a: (a - b + nu * bands) % nu == 0)
    u_right = [dot(unit[c], of_band_t).astype(BF16) for c in range(2)]
    e_right = [[dot(e_ref[q, c], of_mode_t).astype(BF16) for c in range(2)] for q in range(qd)]
    for t in range(tiles):
        first = t * LANES
        of_band = picks(LANES, bands, lambda a, b: (a + first >= nu * b) & (a + first < nu * b + nu))
        of_mode = picks(LANES, nu, lambda a, b: (a + first - b + nu * bands) % nu == 0)
        ur, ui = [dot(of_band, m) for m in u_right]
        for q in range(qd):
            er, ei = [dot(of_mode, m) for m in e_right[q]]
            w_buf[q, 0, first : first + LANES, :] = (ur * er - ui * ei).astype(BF16)
            w_buf[q, 1, first : first + LANES, :] = (ur * ei + ui * er).astype(BF16)

    col = iota((bands, rows), 1)
    slot = col % RB
    m_of = ((col // RB) % n_pb) * M + slot % M
    pick_m = jnp.where(iota((bands, rows), 0) == m_of, 1.0, 0.0).astype(BF16)
    real_in = (slot // M) % 2 == 0
    blocks = []
    for q in range(qd):
        a_r, a_i = [dot(v_ref[q, c], pick_m, ((0,), (0,))) for c in range(2)]
        mine = slot // (2 * M) == q
        blocks.append(jnp.where(mine, jnp.where(real_in, a_r, a_i), 0.0))
        blocks.append(jnp.where(mine, jnp.where(real_in, -a_i, a_r), 0.0))
    v_left = jnp.concatenate(blocks, axis=0).astype(BF16)

    def f_wait(k, c):
        peer, to = place(k)
        pltpu.make_async_remote_copy(
            src_ref=send.at[peer], dst_ref=recv.at[peer], send_sem=s_sem.at[peer],
            recv_sem=r_sem.at[peer], device_id=to, device_id_type=MESH,
        ).wait_recv()
        f_copy(k).wait_send()
        return c

    lax.fori_loop(1, n, f_wait, 0)

    y = dot(v_left, recv[...].reshape(rows, cols)).astype(BF16)
    for q in range(qd):
        yq = y[2 * bands * q : 2 * bands * (q + 1)]
        a = dot(yq, w_buf[q, 0])
        b = dot(yq, w_buf[q, 1])
        o_ref[q, 0] = a[:bands] - b[bands:]
        o_ref[q, 1] = a[bands:] + b[:bands]


def body(wannier_g, rp_coords, q_coords, k_index, k_vectors, kq_vectors, modes):
    n_rp, n_pb = lax.axis_size("rp"), lax.axis_size("pb")
    n = n_rp * n_pb
    qd = q_coords.shape[1]
    _, local, M, cols = wannier_g.shape
    bands, nu = kq_vectors.shape[2], modes.shape[2]
    RB = -(-(qd * 2 * M) // 8) * 8
    paired = M == 2
    tiles = cols // LANES
    right = wannier_g if paired else wannier_g.reshape(2 * local * M, cols)
    g_shape = (tiles, 2, local, M, LANES) if paired else (tiles, 2 * local * M, LANES)
    cfg = (n_rp, n_pb, qd, local, M, cols, bands, nu, RB, paired)
    vmem = pl.BlockSpec(memory_space=pltpu.VMEM)
    smem = pl.BlockSpec(memory_space=pltpu.SMEM)
    return pl.pallas_call(
        functools.partial(kernel, cfg),
        out_shape=jax.ShapeDtypeStruct((qd, 2, bands, cols), F32),
        in_specs=[pl.BlockSpec(memory_space=pl.ANY), vmem, smem, smem, vmem, vmem, vmem],
        out_specs=vmem,
        scratch_shapes=[
            pltpu.VMEM(g_shape, BF16),
            pltpu.VMEM((1, LANES), F32),
            pltpu.VMEM((n, 1, LANES), F32),
            pltpu.VMEM((n, RB, cols), BF16),
            pltpu.VMEM((n, RB, cols), BF16),
            pltpu.VMEM((qd, 2, cols, cols), BF16),
            pltpu.VMEM((LANES, local * M), BF16),
            pltpu.SemaphoreType.DMA((tiles,)),
            pltpu.SemaphoreType.DMA((n,)),
            pltpu.SemaphoreType.DMA((n,)),
            pltpu.SemaphoreType.DMA((n,)),
            pltpu.SemaphoreType.DMA((n,)),
        ],
        compiler_params=pltpu.CompilerParams(
            collective_id=0, has_side_effects=True, vmem_limit_bytes=60 * 2**20
        ),
    )(right, rp_coords, q_coords, k_index, k_vectors, kq_vectors, modes)


def solution(mesh):
    return jax.shard_map(
        body,
        mesh=mesh,
        in_specs=(
            P(None, "rp", "pb", None),
            P(),
            P(None, ("rp", "pb")),
            P(),
            P(),
            P(("rp", "pb"), None, None, None),
            P(("rp", "pb"), None, None, None),
        ),
        out_specs=P(("rp", "pb"), None, None, None),
        check_vma=False,
    )
```

```python
import functools

import jax
import jax.numpy as jnp
import numpy as np
from jax import lax
from jax.experimental import pallas as pl
from jax.experimental.pallas import tpu as pltpu
from jax.sharding import PartitionSpec as P

NK = 16
LANES = 128
MESH = pl.DeviceIdType.MESH
F32 = jnp.float32
BF16 = jnp.bfloat16
ODD = np.linalg.solve(
    np.array([[h, h**3, h**5, h**7] for h in (1.0, 2.0, 3.0, 4.0)]),
    np.sin(np.pi * np.arange(1, 5) / 8.0),
)


def dot(a, b, dims=((1,), (0,))):
    return lax.dot_general(a, b, (dims, ((), ())), preferred_element_type=F32)


def iota(shape, axis):
    return lax.broadcasted_iota(jnp.int32, shape, axis)


def picks(rows, cols, hit):
    return jnp.where(hit(iota((rows, cols), 0), iota((rows, cols), 1)), 1.0, 0.0).astype(BF16)


def wave(sixteenths):
    h = NK // 4 - NK * jnp.abs(sixteenths - jnp.floor(sixteenths + 0.5))
    s = h * h
    return h * (ODD[0] + s * (ODD[1] + s * (ODD[2] + s * ODD[3])))


def wrapped(a, b, size):
    c = a + b
    return jnp.where(c >= size, c - size, c)


def cuts(tiles):
    if tiles < 8:
        return [tiles]
    first, rest = 2, tiles - 2
    sizes = [first] + [rest // 3 + (k < rest % 3) for k in range(3)]
    return sizes


def kernel(
    cfg, g_hbm, rp_hbm, q_ref, k_ref, kv_hbm, v_hbm, e_hbm, o_ref,
    g_buf, rp_ref, kv_ref, v_ref, e_ref, qrow, q_all, xsend, xrecv, red, recv, w_buf, rmat, v_left,
    g_sem, in_sem, qs_sem, qr_sem, xs_sem, xr_sem, s_sem, r_sem,
):
    n_rp, n_pb, qd, local, M, cols, bands, nu, RB, paired = cfg
    n = n_rp * n_pb
    ip, ib = lax.axis_index("rp"), lax.axis_index("pb")
    me = ip * n_pb + ib
    depth = local * M
    half = n_pb * RB
    tiles = cols // LANES

    def to_all(act):
        for dp in range(n_rp):
            p = wrapped(ip, dp, n_rp)

            def one(db, c, p=p):
                act(p, wrapped(ib, db, n_pb))
                return c

            lax.fori_loop(1 if dp == 0 else 0, n_pb, one, 0)

    barrier = pltpu.get_barrier_semaphore()
    to_all(
        lambda p, b: pl.semaphore_signal(barrier, inc=1, device_id=(p, b), device_id_type=MESH)
    )

    inputs = [
        pltpu.make_async_copy(a, b, in_sem.at[k])
        for k, (a, b) in enumerate(
            ((rp_hbm, rp_ref), (kv_hbm, kv_ref), (v_hbm, v_ref), (e_hbm, e_ref))
        )
    ]
    for c in inputs:
        c.start()
    loads = []
    for t in range(tiles):
        lanes = pl.ds(LANES * t, LANES)
        src = g_hbm.at[:, :, :, lanes] if paired else g_hbm.at[:, lanes]
        loads.append(pltpu.make_async_copy(src, g_buf.at[t], g_sem.at[t]))
    for c in loads:
        c.start()

    lane = iota((1, LANES), 1)
    row = jnp.zeros((1, LANES), jnp.int32)
    for d in range(3):
        for j in range(qd):
            row = jnp.where(lane == d * qd + j, q_ref[j, d], row)
    qrow[...] = (row & (NK - 1)).astype(F32)
    q_all[me] = qrow[...]
    for c in inputs:
        c.wait()

    own = rp_ref[:, pl.ds(pl.multiple_of(ip * local, LANES), local)] & (NK - 1)
    spread = picks(local, depth, lambda a, b: a == b // M)
    own = dot((own.astype(F32) * (1.0 / NK)).astype(BF16), spread)
    which = iota((LANES, depth), 0) // qd
    big = jnp.zeros((LANES, depth), F32)
    for d in range(3):
        big = jnp.where(which == d, own[d : d + 1, :], big)
    rmat[...] = big.astype(BF16)

    slot = iota((bands, half), 1) % RB
    m_of = (iota((bands, half), 1) // RB) * M + slot % M
    pick_m = jnp.where(iota((bands, half), 0) == m_of, 1.0, 0.0).astype(BF16)
    real_in = (slot // M) % 2 == 0
    for q in range(qd):
        a_r, a_i = [dot(v_ref[q, c], pick_m, ((0,), (0,))) for c in range(2)]
        mine = slot // (2 * M) == q
        top = jnp.where(mine, jnp.where(real_in, a_r, a_i), 0.0)
        low = jnp.where(mine, jnp.where(real_in, -a_i, a_r), 0.0)
        v_left[2 * bands * q : 2 * bands * (q + 1), :] = jnp.concatenate([top, low], 0).astype(BF16)

    unit = kv_ref[k_ref[0]]
    of_band_t = picks(bands, cols, lambda b, a: (a >= nu * b) & (a < nu * b + nu))
    of_mode_t = picks(nu, cols, lambda b, a: (a - b + nu * bands) % nu == 0)
    u_right = [dot(unit[c], of_band_t).astype(BF16) for c in range(2)]
    e_right = [[dot(e_ref[q, :, c, :], of_mode_t).astype(BF16) for c in range(2)] for q in range(qd)]

    def combine(t):
        first = t * LANES
        of_band = picks(LANES, bands, lambda a, b: (a + first >= nu * b) & (a + first < nu * b + nu))
        of_mode = picks(LANES, nu, lambda a, b: (a + first - b + nu * bands) % nu == 0)
        ur, ui = [dot(of_band, m) for m in u_right]
        for q in range(qd):
            er, ei = [dot(of_mode, m) for m in e_right[q]]
            w_buf[q, 0, first : first + LANES, :] = (ur * er - ui * ei).astype(BF16)
            w_buf[q, 1, first : first + LANES, :] = (ur * ei + ui * er).astype(BF16)

    early = tiles // 2
    for t in range(early):
        combine(t)

    pl.semaphore_wait(barrier, n - 1)

    def q_copy(p, b, slot_of):
        return pltpu.make_async_remote_copy(
            src_ref=qrow, dst_ref=q_all.at[slot_of], send_sem=qs_sem.at[p * n_pb + b],
            recv_sem=qr_sem.at[slot_of], device_id=(p, b), device_id_type=MESH,
        )

    to_all(lambda p, b: q_copy(p, b, me).start())

    def q_done(p, b):
        q_copy(p, b, p * n_pb + b).wait_recv()
        q_copy(p, b, me).wait_send()

    to_all(q_done)

    coords = jnp.concatenate(
        [
            jnp.broadcast_to(q_all[pl.ds(wrapped(ip, dp, n_rp) * n_pb, n_pb)], (n_pb, RB, LANES))
            for dp in range(n_rp)
        ],
        axis=0,
    ).reshape(n * RB, LANES)
    slot = iota((n * RB, LANES), 0) % RB
    coords = jnp.where(iota((n * RB, LANES), 1) % qd == slot // (2 * M), coords, 0.0)
    turns = dot(coords.astype(BF16), rmat[...])
    slot = iota((n * RB, 1), 0) % RB
    imag = (slot // M) % 2 == 1
    keep = (slot % M) == (iota((1, depth), 1) % M)
    left = jnp.concatenate(
        [
            jnp.where(keep, wave(turns + shift), 0.0).astype(BF16)
            for shift in (jnp.where(imag, 0.75, 0.0), jnp.where(imag, 0.0, 0.25))
        ],
        axis=1,
    )

    sizes = cuts(tiles)
    firsts = [sum(sizes[:c]) for c in range(len(sizes))]
    lanes = [slice(LANES * a, LANES * (a + b)) for a, b in zip(firsts, sizes)]

    def x_copy(dp, c):
        part = (slice(None), slice(None), lanes[c])
        return pltpu.make_async_remote_copy(
            src_ref=xsend.at[(dp - 1, *part)], dst_ref=xrecv.at[(dp - 1, *part)],
            send_sem=xs_sem.at[dp - 1, c], recv_sem=xr_sem.at[dp - 1, c],
            device_id=(wrapped(ip, dp, n_rp), ib), device_id_type=MESH,
        )

    def f_copy(b, block, c):
        return pltpu.make_async_remote_copy(
            src_ref=red.at[b, :, lanes[c]], dst_ref=recv.at[block, :, lanes[c]],
            send_sem=s_sem.at[c, b], recv_sem=r_sem.at[c, block],
            device_id=(ip, b), device_id_type=MESH,
        )

    def to_group(act):
        def one(db, c):
            act(wrapped(ib, db, n_pb))
            return c

        lax.fori_loop(1, n_pb, one, 0)

    owned = {}

    def fourier(c):
        parts = []
        for u in range(firsts[c], firsts[c] + sizes[c]):
            loads[u].wait()
            parts.append(g_buf.at[u].reshape(2 * depth, LANES)[...] if paired else g_buf[u])
        right = parts[0] if len(parts) == 1 else jnp.concatenate(parts, axis=1)
        f = dot(left, right)
        owned[c] = f[:half]
        wide = LANES * sizes[c]
        for dp in range(1, n_rp):
            away = f[dp * half : (dp + 1) * half].astype(BF16)
            xsend[dp - 1, :, :, lanes[c]] = away.reshape(n_pb, RB, wide)
            x_copy(dp, c).start()

    def reduce(c):
        total = owned.pop(c)
        wide = LANES * sizes[c]
        for dp in range(1, n_rp):
            x_copy(dp, c).wait()
            total = total + xrecv[dp - 1, :, :, lanes[c]].astype(F32).reshape(half, wide)
        red[:, :, lanes[c]] = total.astype(BF16).reshape(n_pb, RB, wide)
        to_group(lambda b: f_copy(b, ib, c).start())
        recv[ib, :, lanes[c]] = red[ib, :, lanes[c]]

    count = len(sizes)
    fourier(0)
    for c in range(1, count):
        fourier(c)
        if c >= 2:
            reduce(c - 2)
    for c in range(max(count - 2, 0), count):
        reduce(c)
    for t in range(early, tiles):
        combine(t)

    sums = [[0.0, 0.0] for _ in range(qd)]
    for c in range(count):

        def f_done(b, c=c):
            f_copy(b, b, c).wait_recv()
            f_copy(b, ib, c).wait_send()

        to_group(f_done)
        block = recv[:, :, lanes[c]].reshape(half, LANES * sizes[c])
        y = dot(v_left[...], block).astype(BF16)
        for q in range(qd):
            yq = y[2 * bands * q : 2 * bands * (q + 1)]
            for part in range(2):
                sums[q][part] = sums[q][part] + dot(yq, w_buf[q, part, lanes[c], :])
    for q in range(qd):
        a, b = sums[q]
        o_ref[q, 0] = a[:bands] - b[bands:]
        o_ref[q, 1] = a[bands:] + b[:bands]


def body(wannier_g, rp_coords, q_coords, k_index, k_vectors, kq_vectors, modes):
    n_rp, n_pb = lax.axis_size("rp"), lax.axis_size("pb")
    n = n_rp * n_pb
    qd = q_coords.shape[1]
    _, local, M, cols = wannier_g.shape
    bands, nu = kq_vectors.shape[2], modes.shape[2]
    RB = -(-(qd * 2 * M) // 8) * 8
    paired = M == 2
    tiles = cols // LANES
    chunks = len(cuts(tiles))
    right = wannier_g if paired else wannier_g.reshape(2 * local * M, cols)
    g_shape = (tiles, 2, local, M, LANES) if paired else (tiles, 2 * local * M, LANES)
    cfg = (n_rp, n_pb, qd, local, M, cols, bands, nu, RB, paired)
    hbm = pl.BlockSpec(memory_space=pltpu.HBM)
    smem = pl.BlockSpec(memory_space=pltpu.SMEM)
    modes = modes.transpose(0, 2, 1, 3)
    others = max(n_rp - 1, 1)
    return pl.pallas_call(
        functools.partial(kernel, cfg),
        out_shape=jax.ShapeDtypeStruct((qd, 2, bands, cols), F32),
        in_specs=[hbm, hbm, smem, smem, hbm, hbm, hbm],
        out_specs=pl.BlockSpec(memory_space=pltpu.VMEM),
        scratch_shapes=[
            pltpu.VMEM(g_shape, BF16),
            pltpu.VMEM(rp_coords.shape, jnp.int32),
            pltpu.VMEM(k_vectors.shape, BF16),
            pltpu.VMEM(kq_vectors.shape, BF16),
            pltpu.VMEM(modes.shape, BF16),
            pltpu.VMEM((1, LANES), F32),
            pltpu.VMEM((n, 1, LANES), F32),
            pltpu.VMEM((others, n_pb, RB, cols), BF16),
            pltpu.VMEM((others, n_pb, RB, cols), BF16),
            pltpu.VMEM((n_pb, RB, cols), BF16),
            pltpu.VMEM((n_pb, RB, cols), BF16),
            pltpu.VMEM((qd, 2, cols, cols), BF16),
            pltpu.VMEM((LANES, local * M), BF16),
            pltpu.VMEM((qd * 2 * bands, n_pb * RB), BF16),
            pltpu.SemaphoreType.DMA((tiles,)),
            pltpu.SemaphoreType.DMA((4,)),
            pltpu.SemaphoreType.DMA((n,)),
            pltpu.SemaphoreType.DMA((n,)),
            pltpu.SemaphoreType.DMA((others, chunks)),
            pltpu.SemaphoreType.DMA((others, chunks)),
            pltpu.SemaphoreType.DMA((chunks, n_pb)),
            pltpu.SemaphoreType.DMA((chunks, n_pb)),
        ],
        compiler_params=pltpu.CompilerParams(
            collective_id=0, has_side_effects=True, vmem_limit_bytes=60 * 2**20
        ),
    )(right, rp_coords, q_coords.T, k_index, k_vectors, kq_vectors, modes)


def solution(mesh):
    return jax.shard_map(
        body,
        mesh=mesh,
        in_specs=(
            P(None, "rp", "pb", None),
            P(),
            P(None, ("rp", "pb")),
            P(),
            P(),
            P(("rp", "pb"), None, None, None),
            P(("rp", "pb"), None, None, None),
        ),
        out_specs=P(("rp", "pb"), None, None, None),
        check_vma=False,
    )
```

```python
import functools

import jax
import jax.numpy as jnp
import numpy as np
from jax import lax
from jax.experimental import pallas as pl
from jax.experimental.pallas import tpu as pltpu
from jax.sharding import PartitionSpec as P

NK = 16
LANES = 128
MESH = pl.DeviceIdType.MESH
F32 = jnp.float32
BF16 = jnp.bfloat16
ODD = np.linalg.solve(
    np.array([[h, h**3, h**5, h**7] for h in (1.0, 2.0, 3.0, 4.0)]),
    np.sin(np.pi * np.arange(1, 5) / 8.0),
)


def dot(a, b, dims=((1,), (0,))):
    return lax.dot_general(a, b, (dims, ((), ())), preferred_element_type=F32)


def iota(shape, axis):
    return lax.broadcasted_iota(jnp.int32, shape, axis)


def picks(rows, cols, hit):
    return jnp.where(hit(iota((rows, cols), 0), iota((rows, cols), 1)), 1.0, 0.0).astype(BF16)


def wave(sixteenths):
    h = NK // 4 - NK * jnp.abs(sixteenths - jnp.floor(sixteenths + 0.5))
    s = h * h
    return h * (ODD[0] + s * (ODD[1] + s * (ODD[2] + s * ODD[3])))


def wrapped(a, b, size):
    c = a + b
    return jnp.where(c >= size, c - size, c)


def cuts(tiles):
    if tiles < 8:
        return [tiles]
    first, rest = 2, tiles - 2
    sizes = [first] + [rest // 3 + (k < rest % 3) for k in range(3)]
    return sizes


def kernel(
    cfg, g_hbm, rp_hbm, q_ref, k_ref, kv_hbm, v_hbm, e_hbm, o_ref,
    g_buf, rp_ref, kv_ref, v_ref, e_ref, qrow, q_all, xsend, xrecv, red, recv, w_buf, rmat, v_left,
    g_sem, in_sem, qs_sem, qr_sem, xs_sem, xr_sem, s_sem, r_sem,
):
    n_rp, n_pb, qd, local, M, cols, bands, nu, RB, paired = cfg
    n = n_rp * n_pb
    ip, ib = lax.axis_index("rp"), lax.axis_index("pb")
    me = ip * n_pb + ib
    depth = local * M
    half = n_pb * RB
    tiles = cols // LANES

    def to_all(act):
        for dp in range(n_rp):
            p = wrapped(ip, dp, n_rp)

            def one(db, c, p=p):
                act(p, wrapped(ib, db, n_pb))
                return c

            lax.fori_loop(1 if dp == 0 else 0, n_pb, one, 0)

    barrier = pltpu.get_barrier_semaphore()
    to_all(
        lambda p, b: pl.semaphore_signal(barrier, inc=1, device_id=(p, b), device_id_type=MESH)
    )

    inputs = [
        pltpu.make_async_copy(a, b, in_sem.at[k])
        for k, (a, b) in enumerate(
            ((rp_hbm, rp_ref), (kv_hbm, kv_ref), (v_hbm, v_ref), (e_hbm, e_ref))
        )
    ]
    for c in inputs:
        c.start()
    loads = []
    for t in range(tiles):
        lanes = pl.ds(LANES * t, LANES)
        src = g_hbm.at[:, :, :, lanes] if paired else g_hbm.at[:, lanes]
        loads.append(pltpu.make_async_copy(src, g_buf.at[t], g_sem.at[t]))
    for c in loads:
        c.start()

    lane = iota((1, LANES), 1)
    row = jnp.zeros((1, LANES), jnp.int32)
    for d in range(3):
        for j in range(qd):
            row = jnp.where(lane == d * qd + j, q_ref[j, d], row)
    qrow[...] = (row & (NK - 1)).astype(F32)
    q_all[me] = qrow[...]
    for c in inputs:
        c.wait()

    own = rp_ref[:, pl.ds(pl.multiple_of(ip * local, LANES), local)] & (NK - 1)
    spread = picks(local, depth, lambda a, b: a == b // M)
    own = dot((own.astype(F32) * (1.0 / NK)).astype(BF16), spread)
    which = iota((LANES, depth), 0) // qd
    big = jnp.zeros((LANES, depth), F32)
    for d in range(3):
        big = jnp.where(which == d, own[d : d + 1, :], big)
    rmat[...] = big.astype(BF16)

    slot = iota((bands, half), 1) % RB
    m_of = (iota((bands, half), 1) // RB) * M + slot % M
    pick_m = jnp.where(iota((bands, half), 0) == m_of, 1.0, 0.0).astype(BF16)
    real_in = (slot // M) % 2 == 0
    for q in range(qd):
        a_r, a_i = [dot(v_ref[q, c], pick_m, ((0,), (0,))) for c in range(2)]
        mine = slot // (2 * M) == q
        top = jnp.where(mine, jnp.where(real_in, a_r, a_i), 0.0)
        low = jnp.where(mine, jnp.where(real_in, -a_i, a_r), 0.0)
        v_left[2 * bands * q : 2 * bands * (q + 1), :] = jnp.concatenate([top, low], 0).astype(BF16)

    unit = kv_ref[k_ref[0]]
    of_band_t = picks(bands, cols, lambda b, a: (a >= nu * b) & (a < nu * b + nu))
    of_mode_t = picks(nu, cols, lambda b, a: (a - b + nu * bands) % nu == 0)
    u_right = [dot(unit[c], of_band_t).astype(BF16) for c in range(2)]
    e_right = [[dot(e_ref[q, :, c, :], of_mode_t).astype(BF16) for c in range(2)] for q in range(qd)]

    def combine(t):
        first = t * LANES
        of_band = picks(LANES, bands, lambda a, b: (a + first >= nu * b) & (a + first < nu * b + nu))
        of_mode = picks(LANES, nu, lambda a, b: (a + first - b + nu * bands) % nu == 0)
        ur, ui = [dot(of_band, m) for m in u_right]
        for q in range(qd):
            er, ei = [dot(of_mode, m) for m in e_right[q]]
            w_buf[q, 0, first : first + LANES, :] = (ur * er - ui * ei).astype(BF16)
            w_buf[q, 1, first : first + LANES, :] = (ur * ei + ui * er).astype(BF16)

    todo = list(range(tiles))

    def combine_some(most):
        for _ in range(min(most, len(todo))):
            combine(todo.pop(0))

    combine_some(0)

    pl.semaphore_wait(barrier, n - 1)

    def q_copy(p, b, slot_of):
        return pltpu.make_async_remote_copy(
            src_ref=qrow, dst_ref=q_all.at[slot_of], send_sem=qs_sem.at[p * n_pb + b],
            recv_sem=qr_sem.at[slot_of], device_id=(p, b), device_id_type=MESH,
        )

    to_all(lambda p, b: q_copy(p, b, me).start())
    combine_some(3)

    def q_done(p, b):
        q_copy(p, b, p * n_pb + b).wait_recv()
        q_copy(p, b, me).wait_send()

    to_all(q_done)

    coords = jnp.concatenate(
        [
            jnp.broadcast_to(q_all[pl.ds(wrapped(ip, dp, n_rp) * n_pb, n_pb)], (n_pb, RB, LANES))
            for dp in range(n_rp)
        ],
        axis=0,
    ).reshape(n * RB, LANES)
    slot = iota((n * RB, LANES), 0) % RB
    coords = jnp.where(iota((n * RB, LANES), 1) % qd == slot // (2 * M), coords, 0.0)
    turns = dot(coords.astype(BF16), rmat[...])
    slot = iota((n * RB, 1), 0) % RB
    imag = (slot // M) % 2 == 1
    keep = (slot % M) == (iota((1, depth), 1) % M)
    left = jnp.concatenate(
        [
            jnp.where(keep, wave(turns + shift), 0.0).astype(BF16)
            for shift in (jnp.where(imag, 0.75, 0.0), jnp.where(imag, 0.0, 0.25))
        ],
        axis=1,
    )

    sizes = cuts(tiles)
    firsts = [sum(sizes[:c]) for c in range(len(sizes))]
    lanes = [slice(LANES * a, LANES * (a + b)) for a, b in zip(firsts, sizes)]

    def x_copy(dp, c):
        part = (slice(None), slice(None), lanes[c])
        return pltpu.make_async_remote_copy(
            src_ref=xsend.at[(dp - 1, *part)], dst_ref=xrecv.at[(dp - 1, *part)],
            send_sem=xs_sem.at[dp - 1, c], recv_sem=xr_sem.at[dp - 1, c],
            device_id=(wrapped(ip, dp, n_rp), ib), device_id_type=MESH,
        )

    def f_copy(b, block, c):
        return pltpu.make_async_remote_copy(
            src_ref=red.at[b, :, lanes[c]], dst_ref=recv.at[block, :, lanes[c]],
            send_sem=s_sem.at[c, b], recv_sem=r_sem.at[c, block],
            device_id=(ip, b), device_id_type=MESH,
        )

    def to_group(act):
        def one(db, c):
            act(wrapped(ib, db, n_pb))
            return c

        lax.fori_loop(1, n_pb, one, 0)

    owned = {}

    def fourier(c):
        parts = []
        for u in range(firsts[c], firsts[c] + sizes[c]):
            loads[u].wait()
            parts.append(g_buf.at[u].reshape(2 * depth, LANES)[...] if paired else g_buf[u])
        right = parts[0] if len(parts) == 1 else jnp.concatenate(parts, axis=1)
        f = dot(left, right)
        owned[c] = f[:half]
        wide = LANES * sizes[c]
        for dp in range(1, n_rp):
            away = f[dp * half : (dp + 1) * half].astype(BF16)
            xsend[dp - 1, :, :, lanes[c]] = away.reshape(n_pb, RB, wide)
            x_copy(dp, c).start()

    def reduce(c):
        total = owned.pop(c)
        wide = LANES * sizes[c]
        for dp in range(1, n_rp):
            x_copy(dp, c).wait()
            total = total + xrecv[dp - 1, :, :, lanes[c]].astype(F32).reshape(half, wide)
        red[:, :, lanes[c]] = total.astype(BF16).reshape(n_pb, RB, wide)
        to_group(lambda b: f_copy(b, ib, c).start())
        recv[ib, :, lanes[c]] = red[ib, :, lanes[c]]

    count = len(sizes)
    fourier(0)
    for c in range(1, count):
        fourier(c)
        if c >= 2:
            reduce(c - 2)
    for c in range(max(count - 2, 0), count):
        combine_some(1)
        reduce(c)
    combine_some(tiles)

    sums = [[0.0, 0.0] for _ in range(qd)]
    for c in range(count):

        def f_done(b, c=c):
            f_copy(b, b, c).wait_recv()
            f_copy(b, ib, c).wait_send()

        to_group(f_done)
        block = recv[:, :, lanes[c]].reshape(half, LANES * sizes[c])
        y = dot(v_left[...], block).astype(BF16)
        for q in range(qd):
            yq = y[2 * bands * q : 2 * bands * (q + 1)]
            for part in range(2):
                sums[q][part] = sums[q][part] + dot(yq, w_buf[q, part, lanes[c], :])
    for q in range(qd):
        a, b = sums[q]
        o_ref[q, 0] = a[:bands] - b[bands:]
        o_ref[q, 1] = a[bands:] + b[:bands]


def body(wannier_g, rp_coords, q_coords, k_index, k_vectors, kq_vectors, modes):
    n_rp, n_pb = lax.axis_size("rp"), lax.axis_size("pb")
    n = n_rp * n_pb
    qd = q_coords.shape[1]
    _, local, M, cols = wannier_g.shape
    bands, nu = kq_vectors.shape[2], modes.shape[2]
    RB = -(-(qd * 2 * M) // 8) * 8
    paired = M == 2
    tiles = cols // LANES
    chunks = len(cuts(tiles))
    right = wannier_g if paired else wannier_g.reshape(2 * local * M, cols)
    g_shape = (tiles, 2, local, M, LANES) if paired else (tiles, 2 * local * M, LANES)
    cfg = (n_rp, n_pb, qd, local, M, cols, bands, nu, RB, paired)
    hbm = pl.BlockSpec(memory_space=pltpu.HBM)
    smem = pl.BlockSpec(memory_space=pltpu.SMEM)
    modes = modes.transpose(0, 2, 1, 3)
    others = max(n_rp - 1, 1)
    return pl.pallas_call(
        functools.partial(kernel, cfg),
        out_shape=jax.ShapeDtypeStruct((qd, 2, bands, cols), F32),
        in_specs=[hbm, hbm, smem, smem, hbm, hbm, hbm],
        out_specs=pl.BlockSpec(memory_space=pltpu.VMEM),
        scratch_shapes=[
            pltpu.VMEM(g_shape, BF16),
            pltpu.VMEM(rp_coords.shape, jnp.int32),
            pltpu.VMEM(k_vectors.shape, BF16),
            pltpu.VMEM(kq_vectors.shape, BF16),
            pltpu.VMEM(modes.shape, BF16),
            pltpu.VMEM((1, LANES), F32),
            pltpu.VMEM((n, 1, LANES), F32),
            pltpu.VMEM((others, n_pb, RB, cols), BF16),
            pltpu.VMEM((others, n_pb, RB, cols), BF16),
            pltpu.VMEM((n_pb, RB, cols), BF16),
            pltpu.VMEM((n_pb, RB, cols), BF16),
            pltpu.VMEM((qd, 2, cols, cols), BF16),
            pltpu.VMEM((LANES, local * M), BF16),
            pltpu.VMEM((qd * 2 * bands, n_pb * RB), BF16),
            pltpu.SemaphoreType.DMA((tiles,)),
            pltpu.SemaphoreType.DMA((4,)),
            pltpu.SemaphoreType.DMA((n,)),
            pltpu.SemaphoreType.DMA((n,)),
            pltpu.SemaphoreType.DMA((others, chunks)),
            pltpu.SemaphoreType.DMA((others, chunks)),
            pltpu.SemaphoreType.DMA((chunks, n_pb)),
            pltpu.SemaphoreType.DMA((chunks, n_pb)),
        ],
        compiler_params=pltpu.CompilerParams(
            collective_id=0, has_side_effects=True, vmem_limit_bytes=60 * 2**20
        ),
    )(right, rp_coords, q_coords.T, k_index, k_vectors, kq_vectors, modes)


def solution(mesh):
    return jax.shard_map(
        body,
        mesh=mesh,
        in_specs=(
            P(None, "rp", "pb", None),
            P(),
            P(None, ("rp", "pb")),
            P(),
            P(),
            P(("rp", "pb"), None, None, None),
            P(("rp", "pb"), None, None, None),
        ),
        out_specs=P(("rp", "pb"), None, None, None),
        check_vma=False,
    )
```

```python
import functools

import jax
import jax.numpy as jnp
import numpy as np
from jax import lax
from jax.experimental import pallas as pl
from jax.experimental.pallas import tpu as pltpu
from jax.sharding import PartitionSpec as P

NK = 16
LANES = 128
MESH = pl.DeviceIdType.MESH
F32 = jnp.float32
BF16 = jnp.bfloat16
ODD = np.linalg.solve(
    np.array([[h, h**3, h**5, h**7] for h in (1.0, 2.0, 3.0, 4.0)]),
    np.sin(np.pi * np.arange(1, 5) / 8.0),
)


def dot(a, b, dims=((1,), (0,))):
    return lax.dot_general(a, b, (dims, ((), ())), preferred_element_type=F32)


def iota(shape, axis):
    return lax.broadcasted_iota(jnp.int32, shape, axis)


def picks(rows, cols, hit):
    return jnp.where(hit(iota((rows, cols), 0), iota((rows, cols), 1)), 1.0, 0.0).astype(BF16)


def wave(sixteenths):
    h = NK // 4 - NK * jnp.abs(sixteenths - jnp.floor(sixteenths + 0.5))
    s = h * h
    return h * (ODD[0] + s * (ODD[1] + s * (ODD[2] + s * ODD[3])))


def wrapped(a, b, size):
    c = a + b
    return jnp.where(c >= size, c - size, c)


def cuts(tiles):
    if tiles < 8:
        return [tiles]
    first, rest = 2, tiles - 2
    sizes = [first] + [rest // 3 + (k < rest % 3) for k in range(3)]
    return sizes


def kernel(
    cfg, g_hbm, rp_hbm, q_ref, k_ref, kv_hbm, v_hbm, e_hbm, o_ref,
    g_buf, rp_ref, kv_ref, v_ref, e_ref, qrow, q_all, xsend, xrecv, red, recv, w_buf, rmat, v_left,
    g_sem, in_sem, qs_sem, qr_sem, xs_sem, xr_sem, s_sem, r_sem,
):
    n_rp, n_pb, qd, local, M, cols, bands, nu, RB, paired = cfg
    n = n_rp * n_pb
    ip, ib = lax.axis_index("rp"), lax.axis_index("pb")
    me = ip * n_pb + ib
    depth = local * M
    half = n_pb * RB
    tiles = cols // LANES

    def to_all(act):
        for dp in range(n_rp):
            p = wrapped(ip, dp, n_rp)

            def one(db, c, p=p):
                act(p, wrapped(ib, db, n_pb))
                return c

            lax.fori_loop(1 if dp == 0 else 0, n_pb, one, 0)

    barrier = pltpu.get_barrier_semaphore()
    to_all(
        lambda p, b: pl.semaphore_signal(barrier, inc=1, device_id=(p, b), device_id_type=MESH)
    )

    inputs = [
        pltpu.make_async_copy(a, b, in_sem.at[k])
        for k, (a, b) in enumerate(
            ((rp_hbm, rp_ref), (kv_hbm, kv_ref), (v_hbm, v_ref), (e_hbm, e_ref))
        )
    ]
    for c in inputs:
        c.start()
    loads = []
    for t in range(tiles):
        lanes = pl.ds(LANES * t, LANES)
        src = g_hbm.at[:, :, :, lanes] if paired else g_hbm.at[:, lanes]
        loads.append(pltpu.make_async_copy(src, g_buf.at[t], g_sem.at[t]))
    for c in loads:
        c.start()

    lane = iota((1, LANES), 1)
    row = jnp.zeros((1, LANES), jnp.int32)
    for d in range(3):
        for j in range(qd):
            row = jnp.where(lane == d * qd + j, q_ref[j, d], row)
    qrow[...] = (row & (NK - 1)).astype(F32)
    q_all[me] = qrow[...]
    for c in inputs:
        c.wait()

    own = rp_ref[:, pl.ds(pl.multiple_of(ip * local, LANES), local)] & (NK - 1)
    spread = picks(local, depth, lambda a, b: a == b // M)
    own = dot((own.astype(F32) * (1.0 / NK)).astype(BF16), spread)
    which = iota((LANES, depth), 0) // qd
    big = jnp.zeros((LANES, depth), F32)
    for d in range(3):
        big = jnp.where(which == d, own[d : d + 1, :], big)
    rmat[...] = big.astype(BF16)

    slot = iota((bands, half), 1) % RB
    m_of = (iota((bands, half), 1) // RB) * M + slot % M
    pick_m = jnp.where(iota((bands, half), 0) == m_of, 1.0, 0.0).astype(BF16)
    real_in = (slot // M) % 2 == 0
    for q in range(qd):
        a_r, a_i = [dot(v_ref[q, c], pick_m, ((0,), (0,))) for c in range(2)]
        mine = slot // (2 * M) == q
        top = jnp.where(mine, jnp.where(real_in, a_r, a_i), 0.0)
        low = jnp.where(mine, jnp.where(real_in, -a_i, a_r), 0.0)
        v_left[2 * bands * q : 2 * bands * (q + 1), :] = jnp.concatenate([top, low], 0).astype(BF16)

    unit = kv_ref[k_ref[0]]
    of_band_t = picks(bands, cols, lambda b, a: (a >= nu * b) & (a < nu * b + nu))
    of_mode_t = picks(nu, cols, lambda b, a: (a - b + nu * bands) % nu == 0)
    u_right = [dot(unit[c], of_band_t).astype(BF16) for c in range(2)]
    e_right = [[dot(e_ref[q, :, c, :], of_mode_t).astype(BF16) for c in range(2)] for q in range(qd)]

    def combine(t):
        first = t * LANES
        of_band = picks(LANES, bands, lambda a, b: (a + first >= nu * b) & (a + first < nu * b + nu))
        of_mode = picks(LANES, nu, lambda a, b: (a + first - b + nu * bands) % nu == 0)
        ur, ui = [dot(of_band, m) for m in u_right]
        for q in range(qd):
            er, ei = [dot(of_mode, m) for m in e_right[q]]
            w_buf[q, 0, first : first + LANES, :] = (ur * er - ui * ei).astype(BF16)
            w_buf[q, 1, first : first + LANES, :] = (ur * ei + ui * er).astype(BF16)

    todo = list(range(tiles))

    def combine_some(most):
        for _ in range(min(most, len(todo))):
            combine(todo.pop(0))

    combine_some(0)

    pl.semaphore_wait(barrier, n - 1)

    def q_copy(p, b, slot_of):
        return pltpu.make_async_remote_copy(
            src_ref=qrow, dst_ref=q_all.at[slot_of], send_sem=qs_sem.at[p * n_pb + b],
            recv_sem=qr_sem.at[slot_of], device_id=(p, b), device_id_type=MESH,
        )

    to_all(lambda p, b: q_copy(p, b, me).start())
    combine_some(3)

    def q_done(p, b):
        q_copy(p, b, p * n_pb + b).wait_recv()
        q_copy(p, b, me).wait_send()

    to_all(q_done)

    coords = jnp.concatenate(
        [
            jnp.broadcast_to(q_all[pl.ds(wrapped(ip, dp, n_rp) * n_pb, n_pb)], (n_pb, RB, LANES))
            for dp in range(n_rp)
        ],
        axis=0,
    ).reshape(n * RB, LANES)
    slot = iota((n * RB, LANES), 0) % RB
    coords = jnp.where(iota((n * RB, LANES), 1) % qd == slot // (2 * M), coords, 0.0)
    turns = dot(coords.astype(BF16), rmat[...])
    slot = iota((n * RB, 1), 0) % RB
    imag = (slot // M) % 2 == 1
    keep = (slot % M) == (iota((1, depth), 1) % M)
    left = jnp.concatenate(
        [
            jnp.where(keep, wave(turns + shift), 0.0).astype(BF16)
            for shift in (jnp.where(imag, 0.75, 0.0), jnp.where(imag, 0.0, 0.25))
        ],
        axis=1,
    )

    sizes = cuts(tiles)
    firsts = [sum(sizes[:c]) for c in range(len(sizes))]
    lanes = [slice(LANES * a, LANES * (a + b)) for a, b in zip(firsts, sizes)]

    def x_copy(dp, c):
        part = (slice(None), slice(None), lanes[c])
        return pltpu.make_async_remote_copy(
            src_ref=xsend.at[(dp - 1, *part)], dst_ref=xrecv.at[(dp - 1, *part)],
            send_sem=xs_sem.at[dp - 1, c], recv_sem=xr_sem.at[dp - 1, c],
            device_id=(wrapped(ip, dp, n_rp), ib), device_id_type=MESH,
        )

    def f_copy(b, block, c):
        return pltpu.make_async_remote_copy(
            src_ref=red.at[b, :, lanes[c]], dst_ref=recv.at[block, :, lanes[c]],
            send_sem=s_sem.at[c, b], recv_sem=r_sem.at[c, block],
            device_id=(ip, b), device_id_type=MESH,
        )

    def to_group(act):
        def one(db, c):
            act(wrapped(ib, db, n_pb))
            return c

        lax.fori_loop(1, n_pb, one, 0)

    owned = {}

    def fourier(c):
        parts = []
        for u in range(firsts[c], firsts[c] + sizes[c]):
            loads[u].wait()
            parts.append(g_buf.at[u].reshape(2 * depth, LANES)[...] if paired else g_buf[u])
        right = parts[0] if len(parts) == 1 else jnp.concatenate(parts, axis=1)
        f = dot(left, right)
        owned[c] = f[:half]
        wide = LANES * sizes[c]
        for dp in range(1, n_rp):
            away = f[dp * half : (dp + 1) * half].astype(BF16)
            xsend[dp - 1, :, :, lanes[c]] = away.reshape(n_pb, RB, wide)
            x_copy(dp, c).start()

    def reduce(c):
        total = owned.pop(c)
        wide = LANES * sizes[c]
        for dp in range(1, n_rp):
            x_copy(dp, c).wait()
            total = total + xrecv[dp - 1, :, :, lanes[c]].astype(F32).reshape(half, wide)
        red[:, :, lanes[c]] = total.astype(BF16).reshape(n_pb, RB, wide)
        to_group(lambda b: f_copy(b, ib, c).start())
        recv[ib, :, lanes[c]] = red[ib, :, lanes[c]]

    count = len(sizes)
    fourier(0)
    for c in range(1, count):
        fourier(c)
        if c >= 2:
            reduce(c - 2)
    for c in range(max(count - 2, 0), count):
        combine_some(1 + (c == count - 1))
        reduce(c)
    combine_some(tiles)

    sums = [[0.0, 0.0] for _ in range(qd)]
    for c in range(count):

        def f_done(b, c=c):
            f_copy(b, b, c).wait_recv()
            f_copy(b, ib, c).wait_send()

        to_group(f_done)
        block = recv[:, :, lanes[c]].reshape(half, LANES * sizes[c])
        y = dot(v_left[...], block).astype(BF16)
        for q in range(qd):
            yq = y[2 * bands * q : 2 * bands * (q + 1)]
            for part in range(2):
                sums[q][part] = sums[q][part] + dot(yq, w_buf[q, part, lanes[c], :])
    for q in range(qd):
        a, b = sums[q]
        o_ref[q, 0] = a[:bands] - b[bands:]
        o_ref[q, 1] = a[bands:] + b[:bands]


def body(wannier_g, rp_coords, q_coords, k_index, k_vectors, kq_vectors, modes):
    n_rp, n_pb = lax.axis_size("rp"), lax.axis_size("pb")
    n = n_rp * n_pb
    qd = q_coords.shape[1]
    _, local, M, cols = wannier_g.shape
    bands, nu = kq_vectors.shape[2], modes.shape[2]
    RB = -(-(qd * 2 * M) // 8) * 8
    paired = M == 2
    tiles = cols // LANES
    chunks = len(cuts(tiles))
    right = wannier_g if paired else wannier_g.reshape(2 * local * M, cols)
    g_shape = (tiles, 2, local, M, LANES) if paired else (tiles, 2 * local * M, LANES)
    cfg = (n_rp, n_pb, qd, local, M, cols, bands, nu, RB, paired)
    hbm = pl.BlockSpec(memory_space=pltpu.HBM)
    smem = pl.BlockSpec(memory_space=pltpu.SMEM)
    modes = modes.transpose(0, 2, 1, 3)
    others = max(n_rp - 1, 1)
    return pl.pallas_call(
        functools.partial(kernel, cfg),
        out_shape=jax.ShapeDtypeStruct((qd, 2, bands, cols), F32),
        in_specs=[hbm, hbm, smem, smem, hbm, hbm, hbm],
        out_specs=pl.BlockSpec(memory_space=pltpu.VMEM),
        scratch_shapes=[
            pltpu.VMEM(g_shape, BF16),
            pltpu.VMEM(rp_coords.shape, jnp.int32),
            pltpu.VMEM(k_vectors.shape, BF16),
            pltpu.VMEM(kq_vectors.shape, BF16),
            pltpu.VMEM(modes.shape, BF16),
            pltpu.VMEM((1, LANES), F32),
            pltpu.VMEM((n, 1, LANES), F32),
            pltpu.VMEM((others, n_pb, RB, cols), BF16),
            pltpu.VMEM((others, n_pb, RB, cols), BF16),
            pltpu.VMEM((n_pb, RB, cols), BF16),
            pltpu.VMEM((n_pb, RB, cols), BF16),
            pltpu.VMEM((qd, 2, cols, cols), BF16),
            pltpu.VMEM((LANES, local * M), BF16),
            pltpu.VMEM((qd * 2 * bands, n_pb * RB), BF16),
            pltpu.SemaphoreType.DMA((tiles,)),
            pltpu.SemaphoreType.DMA((4,)),
            pltpu.SemaphoreType.DMA((n,)),
            pltpu.SemaphoreType.DMA((n,)),
            pltpu.SemaphoreType.DMA((others, chunks)),
            pltpu.SemaphoreType.DMA((others, chunks)),
            pltpu.SemaphoreType.DMA((chunks, n_pb)),
            pltpu.SemaphoreType.DMA((chunks, n_pb)),
        ],
        compiler_params=pltpu.CompilerParams(
            collective_id=0, has_side_effects=True, vmem_limit_bytes=60 * 2**20
        ),
    )(right, rp_coords, q_coords.T, k_index, k_vectors, kq_vectors, modes)


def solution(mesh):
    return jax.shard_map(
        body,
        mesh=mesh,
        in_specs=(
            P(None, "rp", "pb", None),
            P(),
            P(None, ("rp", "pb")),
            P(),
            P(),
            P(("rp", "pb"), None, None, None),
            P(("rp", "pb"), None, None, None),
        ),
        out_specs=P(("rp", "pb"), None, None, None),
        check_vma=False,
    )
```
